512 devices in a mesh: gx: 4 (over y_lo), gy: 128 (over z, y_hi, x, core).
Axes of the slice: x: 4, y: 8 (y_hi: 2, y_lo: 4; y = y_hi * 4 + y_lo), z: 8, core: 2. Of those that a mesh axis runs over, the one named last changes fastest.
Arguments:
- traces: bfloat16 [8, 256, 128, 256], P('gx', 'gy'), may hold values from -6 to 6
- aperture: int32 [8, 256, 9], P('gx', 'gy'), may hold values 0 or 1
- geometry: int32 [8, 256, 3, 128], P('gx', 'gy'), may hold values from 0 to 1023, as said below
- trace_weight: bfloat16 [8, 256, 128], P('gx', 'gy'), may hold values from 0.0087890625 to 0.03515625
- class_weight: float32 [14], replicated, may hold values from 0.3 to 1.5
- traveltime: int32 [14, 256], replicated, may hold values from 0 to 1114
Outputs:
- image: float32 [64, 1024, 256], P('gx', 'gy')
The draws below stay inside these ranges and needn't reach their ends.
Inputs may be any that keep to these rules, and one draw needn't show every extreme that they name: Row 0 of a trace's geometry is an inline midpoint among the 16 image columns of its block's tile, row 1 a crossline midpoint among its tile's 8 columns, row 2 an offset class below 8.
All inputs are finite; a program needn't handle non-finite values. No bound on the sum of `aperture` on one device may be relied on, other than what follows from the above.
Results may differ from the reference program's by a relative error of at most 0.0029.
Values may be sent and summed in bfloat16 or wider, within the bound.
A program may use at most 64 MiB of HBM per device.

```python
import math
import jax
import jax.numpy as jnp
from jax import lax

NS = 256
NTIME = 256
TR = 128
NH = 8
BB = 2
PX = 16
PY = 8
DSTEP = 8
NC = 14
NBX = 8
NBY = 256
NX = 64
NY = 1024
N_GX = 4
N_GY = 128


def draw_geometry(key, part):
    keys = jax.random.split(jax.random.fold_in(key, 11), 3)
    block_x = jnp.arange(NBX, dtype=jnp.int32)[:, None, None] // BB
    block_y = jnp.arange(NBY, dtype=jnp.int32)[None, :, None] // BB
    inline = block_x * PX + jax.random.randint(keys[0], (NBX, NBY, TR), 0, PX)
    crossline = block_y * PY + jax.random.randint(keys[1], (NBX, NBY, TR), 0, PY)
    offset_class = jax.random.randint(keys[2], (NBX, NBY, TR), 0, NH)
    return jnp.stack([inline, crossline, offset_class], axis=2).astype(jnp.int32)


def draw_traveltime(key, part):
    level = jnp.arange(NC, dtype=jnp.int32)[:, None]
    sample = jnp.arange(NTIME, dtype=jnp.int32)[None, :]
    raw = jax.random.randint(jax.random.fold_in(key, 23), (NC, NTIME), 0, 1 << 20)
    extra = raw % (4 * level + 4)
    return (4 * sample + 3 * level + extra).astype(jnp.int32)


def touch_ends(entries, key, low, high):
    extent = entries.shape
    index_at = [jax.random.randint(jax.random.fold_in(key, axis), (), 0, extent[axis]) for axis in range(len(extent))]
    entries = entries.at[tuple(index_at)].set(low)
    longest = extent.index(max(extent))
    index_at[longest] = (index_at[longest] + 1) % extent[longest]
    return entries.at[tuple(index_at)].set(high)


def levels(stream_key, dims, pieces, least, largest):
    gain = 1.0
    for axis_at, blocks in pieces:
        steps = jax.random.uniform(jax.random.fold_in(jax.random.fold_in(stream_key, 6), axis_at), (blocks,), jnp.float32, least / len(pieces), largest / len(pieces))
        gain = gain * jnp.repeat(jnp.exp(steps), dims[axis_at] // blocks).reshape((-1,) + (1,) * (len(dims) - 1 - axis_at))
    return gain


def scatter_about(stream_key, dims, deviation, bound, cuts=(), kind=jnp.bfloat16):
    result = deviation * jax.random.normal(stream_key, dims, jnp.float32)
    if cuts:
        result = result * levels(stream_key, dims, cuts, -0.22, 0.18)
    return jnp.clip(result, -bound, bound).astype(kind)


def setup_inputs(seed: int = 0) -> dict:
    streams_of = jax.random.split(jax.random.key(seed), 7)
    return {
        "traces": scatter_about(streams_of[0], (NBX, NBY, TR, NS), 1.0, 6.0, ((0, 4), (1, 128))),
        "aperture": touch_ends((jax.random.randint(streams_of[1], (NBX, NBY, 9), 0, 3) < 2).astype(jnp.int32), jax.random.fold_in(streams_of[1], 1), 0, 1),
        "geometry": draw_geometry(jax.random.fold_in(streams_of[6], 71), 0),
        "trace_weight": jnp.clip(jnp.exp(math.log(0.03515625) - 1.3862944 * jax.random.uniform(streams_of[3], (NBX, NBY, TR), jnp.float32) ** levels(streams_of[3], (NBX, NBY, TR), ((0, 4), (1, 128)), -0.2, 0.2)), 0.0087890625, 0.03515625).astype(jnp.bfloat16),
        "class_weight": jnp.clip(jnp.exp(jax.random.uniform(streams_of[4], (NC,), jnp.float32, math.log(0.3), math.log(1.5))), 0.3, 1.5),
        "traveltime": draw_traveltime(jax.random.fold_in(streams_of[6], 71), 0),
    }


def migrate(samples_in, live_weights, geometry, tile_x, tile_y, traveltime, class_weight):
    points = jnp.arange(PX * PY, dtype=jnp.int32)
    point_x = tile_x * PX + points // PY
    point_y = tile_y * PY + points % PY
    distance = jnp.abs(point_x[:, None] - geometry[0][None, :]) + jnp.abs(point_y[:, None] - geometry[1][None, :])
    classes = geometry[2][None, :] + distance // DSTEP
    sample_ids = jnp.arange(NS, dtype=jnp.int32)[:, None]
    samples_wide = samples_in.astype(jnp.float32)

    def add_class(level, image):
        scaled = (live_weights * class_weight[level]).astype(jnp.bfloat16).astype(jnp.float32)
        amplitude = jnp.where(classes == level, scaled[None, :], jnp.float32(0.0))
        stacked = jnp.dot(amplitude, samples_wide, precision=lax.Precision.HIGHEST, preferred_element_type=jnp.float32)
        quarter = traveltime[level]
        first_sample = quarter // 4
        fraction = (quarter % 4).astype(jnp.float32) * 0.25
        interp = jnp.where(sample_ids == first_sample[None, :], 1.0 - fraction[None, :], 0.0) + jnp.where(sample_ids == first_sample[None, :] + 1, fraction[None, :], 0.0)
        return image + jnp.dot(stacked, interp.astype(jnp.float32), precision=lax.Precision.HIGHEST, preferred_element_type=jnp.float32)

    return lax.fori_loop(0, class_weight.shape[0], add_class, jnp.zeros((PX * PY, NTIME), jnp.float32))


def reference(traces, aperture, geometry, trace_weight, class_weight, traveltime):
    padded_traces = jnp.pad(traces, ((BB, BB), (BB, BB), (0, 0), (0, 0)))
    padded_aperture = jnp.pad(aperture, ((BB, BB), (BB, BB), (0, 0)))
    padded_geometry = jnp.pad(geometry, ((BB, BB), (BB, BB), (0, 0), (0, 0)))
    padded_weight = jnp.pad(trace_weight, ((BB, BB), (BB, BB), (0, 0)))
    offset = jnp.arange(3 * BB, dtype=jnp.int32) // BB - 1
    wanted = (1 - offset)[:, None] * 3 + (1 - offset)[None, :]
    choose = (jnp.arange(9, dtype=jnp.int32)[None, None, :] == wanted[:, :, None]).astype(jnp.int32)
    zero_index = jnp.int32(0)

    def one_tile(tile):
        tile_x = (tile // N_GY).astype(jnp.int32)
        tile_y = (tile % N_GY).astype(jnp.int32)
        start_x = (tile_x * BB).astype(jnp.int32)
        start_y = (tile_y * BB).astype(jnp.int32)
        near_traces = lax.dynamic_slice(padded_traces, (start_x, start_y, zero_index, zero_index), (3 * BB, 3 * BB, TR, NS))
        near_aperture = lax.dynamic_slice(padded_aperture, (start_x, start_y, zero_index), (3 * BB, 3 * BB, 9))
        near_geometry = lax.dynamic_slice(padded_geometry, (start_x, start_y, zero_index, zero_index), (3 * BB, 3 * BB, 3, TR))
        near_weight = lax.dynamic_slice(padded_weight, (start_x, start_y, zero_index), (3 * BB, 3 * BB, TR))
        live_block = jnp.sum(near_aperture * choose, axis=2)
        live = jnp.broadcast_to(live_block[:, :, None], near_weight.shape).reshape(-1)
        live_weights = near_weight.reshape(-1).astype(jnp.float32) * live.astype(jnp.float32)
        flat_geometry = jnp.moveaxis(near_geometry, 2, 0).reshape(3, -1)
        return migrate(near_traces.reshape(-1, NS), live_weights, flat_geometry, tile_x, tile_y, traveltime, class_weight)

    tiles = lax.map(one_tile, jnp.arange(N_GX * N_GY, dtype=jnp.int32))
    return tiles.reshape(N_GX, N_GY, PX, PY, NTIME).transpose(0, 2, 1, 3, 4).reshape(NX, NY, NTIME)
```

```python
import jax
import jax.numpy as jnp
from jax import lax
from jax.experimental import pallas as pl
from jax.experimental.pallas import tpu as pltpu
from jax.sharding import PartitionSpec as P

NS = 256
NT = 256
TR = 128
NB = 4
NJ = NB * TR
NC = 14
NOC = 8
PX = 16
PY = 8
PTS = PX * PY
L_OWN, L_X, L_Y, L_XY = 3, 5, 4, 6
LV = 7
MESH = pl.DeviceIdType.MESH
BF = jnp.bfloat16
F32 = jnp.float32


def kernel(
    tr_ref, ap_ref, geo_ref, wt_ref, cw_ref, tt_ref, out_ref,
    t_ref, v_ref, a_ref, fo, fx, acc, so, sp, sx, sf, ro, rp, rx, rf, send, recv,
):
    gx = lax.axis_index("gx")
    gy = lax.axis_index("gy")
    ngx = lax.axis_size("gx")
    ngy = lax.axis_size("gy")
    core = lax.rem(gy, 2)
    step = 2 * core - 1
    partner = gy - step
    far = gy + step
    has_lo = gx > 0
    has_hi = gx < ngx - 1
    has_far = jnp.logical_and(far >= 0, far < ngy)

    barrier = pltpu.get_barrier_semaphore()

    def greet(dev):
        pl.semaphore_signal(barrier, inc=1, device_id=dev, device_id_type=MESH)

    pl.when(has_far)(lambda: greet((gx, far)))
    pl.when(has_lo)(lambda: greet((gx - 1, gy)))
    pl.when(has_hi)(lambda: greet((gx + 1, gy)))
    greet((gx, partner))

    def copy(src, dst, k, dev):
        return pltpu.make_async_remote_copy(
            src_ref=src, dst_ref=dst, send_sem=send.at[k], recv_sem=recv.at[k], device_id=dev, device_id_type=MESH
        )

    lo, hi, pa, fa = (gx - 1, gy), (gx + 1, gy), (gx, partner), (gx, far)
    to_hi_o = copy(so.at[1], ro.at[0], 0, hi)
    to_lo_o = copy(so.at[0], ro.at[1], 1, lo)
    to_pa = copy(sp, rp, 2, pa)
    to_hi_x = copy(sx.at[1], rx.at[0], 3, hi)
    to_lo_x = copy(sx.at[0], rx.at[1], 4, lo)
    to_fa = copy(sf, rf, 5, fa)

    traces = tr_ref[...]
    sample = lax.broadcasted_iota(jnp.int32, (NS, NT), 0).astype(F32).astype(BF)
    zero = jnp.zeros((NS, NT), BF)
    for c in range(NC):
        q = tt_ref[c : c + 1, :]
        first = q // 4
        frac = (q % 4).astype(F32) * 0.25
        s0 = jnp.broadcast_to(first.astype(F32), (NS, NT)).astype(BF)
        s1 = jnp.broadcast_to((first + 1).astype(F32), (NS, NT)).astype(BF)
        w1 = jnp.broadcast_to(frac, (NS, NT)).astype(BF)
        w0 = jnp.broadcast_to(1.0 - frac, (NS, NT)).astype(BF)
        interp = jnp.where(sample == s0, w0, jnp.where(sample == s1, w1, zero))
        t_ref[c] = jnp.dot(traces, interp, preferred_element_type=F32).astype(BF)

    for b in range(NB):
        i, k = b // 2, b % 2
        oc_row = jnp.broadcast_to(geo_ref[i, k, 2:3, :], (TR, TR)).astype(F32)
        oc = jnp.transpose(oc_row)
        oc = jnp.concatenate([oc, oc], axis=1).astype(BF)
        for r in range(0, TR, 16):
            o = oc[r : r + 16]
            row = b * TR + r
            b2 = o >= 4
            o = jnp.where(b2, o - 4, o)
            b1 = o >= 2
            o = jnp.where(b1, o - 2, o)
            b0 = o >= 1
            t = [t_ref[c, row : row + 16, :] for c in range(NC)]
            t = [jnp.where(b2, t[c + 4], t[c]) for c in range(NC - 4)]
            t = [jnp.where(b1, t[c + 2], t[c]) for c in range(NC - 6)]
            t = [jnp.where(b0, t[c + 1], t[c]) for c in range(NC - 7)]
            for d in range(LV):
                v_ref[d * NJ + row : d * NJ + row + 16, :] = t[d]

    row16 = lax.broadcasted_iota(jnp.int32, (16, TR), 0)
    upper = (row16 // 8).astype(F32) * 0.125
    py = (row16 % 8).astype(F32) * 0.125
    ex, ey, wd = [], [], []
    for b in range(NB):
        i, k = b // 2, b % 2
        mx = (geo_ref[i, k, 0:1, :] - gx * PX).astype(F32) * 0.125
        my = (geo_ref[i, k, 1:2, :] - gy * PY).astype(F32) * 0.125
        ex.append((upper - mx).astype(BF))
        ey.append((py - my).astype(BF))
        oc = geo_ref[i, k, 2:3, :]
        w = wt_ref[i, k : k + 1, :].astype(F32)
        levels = []
        for d in range(LV):
            cw = jnp.zeros((1, TR), F32)
            for o in range(NOC):
                if o + d < NC:
                    cw = jnp.where(oc == o, cw_ref[o + d], cw)
            levels.append(jnp.broadcast_to(w * cw, (16, TR)).astype(BF))
        wd.append(levels)
    zero16 = jnp.zeros((16, TR), BF)

    def live_of(b, dx, kind):
        i, k = b // 2, b % 2
        base = (dx + 1) * 3
        mid = ap_ref[i, k, base + 1]
        up = ap_ref[i, k, base + 2]
        down = ap_ref[i, k, base]
        if kind == 0:
            return mid
        if kind == 1:
            return jnp.where(core == 1, up, down)
        return jnp.where(core == 1, down, up)

    def tile(slot, dx, kind, nlev):
        shift = {0: 0, 1: step, 2: -step}[kind]
        for b in range(NB):
            gone = (1 - live_of(b, dx, kind)).astype(F32) * 64.0
            dy = jnp.abs(ey[b] + shift.astype(F32).astype(BF) if kind else ey[b]) + gone.astype(BF)
            for g in range(PX // 2):
                dist = jnp.abs(ex[b] + jnp.asarray(2 * dx + 0.25 * g, BF)) + dy
                level = jnp.floor(dist)
                for d in range(nlev):
                    a_ref[slot, 16 * g : 16 * g + 16, d * NJ + b * TR : d * NJ + b * TR + TR] = jnp.where(
                        level == d, wd[b][d], zero16
                    )

    def migrate(slot, count, nlev):
        lhs = a_ref[slot : slot + count, :, : nlev * NJ].reshape(count * PTS, nlev * NJ)
        return jnp.dot(lhs, v_ref[: nlev * NJ, :], preferred_element_type=F32)

    tile(0, -1, 1, LV)
    tile(1, 1, 1, LV)
    so[...] = migrate(0, 2, LV).astype(BF).reshape(2, PTS, NT)
    count = has_lo.astype(jnp.int32) + has_hi.astype(jnp.int32) + has_far.astype(jnp.int32) + 1
    pl.semaphore_wait(barrier, count)
    pl.when(has_hi)(lambda: to_hi_o.start())
    pl.when(has_lo)(lambda: to_lo_o.start())
    tile(2, 0, 1, L_Y)
    fo[...] = migrate(2, 1, L_Y)
    tile(3, -1, 2, LV)
    tile(4, 1, 2, LV)
    corners = migrate(3, 2, LV).astype(BF)
    sp[0] = corners[:PTS]
    sp[1] = corners[PTS:]
    tile(5, 0, 2, L_Y)
    sp[2] = migrate(5, 1, L_Y).astype(BF)
    to_pa.start()

    @pl.when(has_lo)
    def _():
        to_hi_o.wait_recv()
        fo[...] += ro[0].astype(F32)

    @pl.when(has_hi)
    def _():
        to_lo_o.wait_recv()
        fo[...] += ro[1].astype(F32)

    @pl.when(has_far)
    def _():
        sf[...] = fo[...].astype(BF)
        to_fa.start()

    tile(6, -1, 0, L_X)
    tile(7, 1, 0, L_X)
    fx[...] = migrate(6, 2, L_X)
    to_pa.wait_recv()
    sx[0] = (fx[:PTS] + rp[0].astype(F32)).astype(BF)
    sx[1] = (fx[PTS:] + rp[1].astype(F32)).astype(BF)
    pl.when(has_hi)(lambda: to_hi_x.start())
    pl.when(has_lo)(lambda: to_lo_x.start())
    tile(8, 0, 0, L_OWN)
    acc[...] = migrate(8, 1, L_OWN) + rp[2].astype(F32)

    @pl.when(has_lo)
    def _():
        to_hi_x.wait_recv()
        acc[...] += rx[0].astype(F32)

    @pl.when(has_hi)
    def _():
        to_lo_x.wait_recv()
        acc[...] += rx[1].astype(F32)

    @pl.when(has_far)
    def _():
        to_fa.wait_recv()
        acc[...] += rf[...].astype(F32)

    out_ref[...] = acc[...].reshape(PX, PY, NT)

    to_pa.wait_send()
    pl.when(has_far)(lambda: to_fa.wait_send())

    @pl.when(has_hi)
    def _():
        to_hi_o.wait_send()
        to_hi_x.wait_send()

    @pl.when(has_lo)
    def _():
        to_lo_o.wait_send()
        to_lo_x.wait_send()


def per_device(traces, aperture, geometry, trace_weight, class_weight, traveltime):
    vmem = pl.BlockSpec(memory_space=pltpu.VMEM)
    smem = pl.BlockSpec(memory_space=pltpu.SMEM)
    tile = (PTS, NT)
    return pl.pallas_call(
        kernel,
        out_shape=jax.ShapeDtypeStruct((PX, PY, NT), F32),
        in_specs=[vmem, smem, vmem, vmem, smem, vmem],
        out_specs=vmem,
        scratch_shapes=[
            pltpu.VMEM((NC, NJ, NT), BF),
            pltpu.VMEM((LV * NJ, NT), BF),
            pltpu.VMEM((9, PTS, LV * NJ), BF),
            pltpu.VMEM(tile, F32),
            pltpu.VMEM((2 * PTS, NT), F32),
            pltpu.VMEM(tile, F32),
            pltpu.VMEM((2,) + tile, BF),
            pltpu.VMEM((3,) + tile, BF),
            pltpu.VMEM((2,) + tile, BF),
            pltpu.VMEM(tile, BF),
            pltpu.VMEM((2,) + tile, BF),
            pltpu.VMEM((3,) + tile, BF),
            pltpu.VMEM((2,) + tile, BF),
            pltpu.VMEM(tile, BF),
            pltpu.SemaphoreType.DMA((6,)),
            pltpu.SemaphoreType.DMA((6,)),
        ],
        compiler_params=pltpu.CompilerParams(
            collective_id=0, has_side_effects=True, vmem_limit_bytes=60 * 1024 * 1024
        ),
        cost_estimate=pl.CostEstimate(flops=3_000_000_000, bytes_accessed=2_000_000, transcendentals=0),
        name="migrate",
    )(traces.reshape(NJ, NS), aperture, geometry, trace_weight, class_weight, traveltime)


def solution(mesh):
    return jax.shard_map(
        per_device,
        mesh=mesh,
        in_specs=(
            P("gx", "gy", None, None),
            P("gx", "gy", None),
            P("gx", "gy", None, None),
            P("gx", "gy", None),
            P(),
            P(),
        ),
        out_specs=P("gx", "gy", None),
        check_vma=False,
    )
```

```python
import jax
import jax.numpy as jnp
from jax import lax
from jax.experimental import pallas as pl
from jax.experimental.pallas import tpu as pltpu
from jax.sharding import PartitionSpec as P

NS = 256
NT = 256
TR = 128
NB = 4
NJ = NB * TR
NC = 14
NOC = 8
PX = 16
PY = 8
PTS = PX * PY
L_OWN, L_X, L_Y, L_XY = 3, 5, 4, 6
LV = 7
MESH = pl.DeviceIdType.MESH
BF = jnp.bfloat16
F32 = jnp.float32


def kernel(
    tr_hbm, ap_hbm, geo_hbm, wt_hbm, cw_hbm, tt_hbm, out_ref,
    tr_ref, ap_ref, geo_ref, wt_ref, cw_ref, tt_ref, i_ref, t_ref, v_ref, a_ref, sent, got, load, send, recv,
):
    gx = lax.axis_index("gx")
    gy = lax.axis_index("gy")
    ngx = lax.axis_size("gx")
    ngy = lax.axis_size("gy")
    core = lax.rem(gy, 2)
    step = 2 * core - 1
    has_x = {-1: gx > 0, 1: gx < ngx - 1, 0: None}
    has_far = jnp.logical_and(gy + step >= 0, gy + step < ngy)

    order = [(0, 1), (-1, 1), (1, 1), (-1, 2), (1, 2), (-1, 0), (1, 0), (0, 2)]

    def device(dx, kind):
        return (gx + dx, gy + {0: 0, 1: step, 2: -step}[kind])

    def exists(dx, kind):
        side = has_x[dx]
        if kind == 1:
            return has_far if side is None else jnp.logical_and(side, has_far)
        return side

    def guarded(cond, body):
        if cond is None:
            body()
        else:
            pl.when(cond)(body)

    barrier = pltpu.get_barrier_semaphore()
    count = jnp.int32(0)
    for n in order:
        cond = exists(*n)
        guarded(
            cond,
            lambda n=n: pl.semaphore_signal(barrier, inc=1, device_id=device(*n), device_id_type=MESH),
        )
        count = count + (1 if cond is None else cond.astype(jnp.int32))

    loads = [
        pltpu.make_async_copy(src, dst, load.at[k])
        for k, (src, dst) in enumerate(
            [(tt_hbm, tt_ref), (geo_hbm, geo_ref), (wt_hbm, wt_ref), (cw_hbm, cw_ref), (ap_hbm, ap_ref), (tr_hbm, tr_ref)]
        )
    ]
    for copy in loads:
        copy.start()

    copies = []
    for k, (dx, kind) in enumerate(order):
        copies.append(
            pltpu.make_async_remote_copy(
                src_ref=sent.at[k],
                dst_ref=got.at[k],
                send_sem=send.at[k],
                recv_sem=recv.at[k],
                device_id=device(dx, kind),
                device_id_type=MESH,
            )
        )

    loads[0].wait()
    sample = lax.broadcasted_iota(jnp.int32, (NS, NT), 0).astype(F32).astype(BF)
    zero = jnp.zeros((NS, NT), BF)
    for c in range(NC):
        q = tt_ref[c : c + 1, :]
        first = q // 4
        frac = (q % 4).astype(F32) * 0.25
        s0 = jnp.broadcast_to(first.astype(F32), (NS, NT)).astype(BF)
        s1 = jnp.broadcast_to((first + 1).astype(F32), (NS, NT)).astype(BF)
        w1 = jnp.broadcast_to(frac, (NS, NT)).astype(BF)
        w0 = jnp.broadcast_to(1.0 - frac, (NS, NT)).astype(BF)
        i_ref[c] = jnp.where(sample == s0, w0, jnp.where(sample == s1, w1, zero))

    for copy in loads[1:5]:
        copy.wait()
    row16 = lax.broadcasted_iota(jnp.int32, (16, TR), 0)
    upper = (row16 // 8).astype(F32) * 0.125
    py = (row16 % 8).astype(F32) * 0.125
    ex, ey, wd = [], [], []
    for b in range(NB):
        i, k = b // 2, b % 2
        mx = (geo_ref[i, 0, k : k + 1, :] - gx * PX).astype(F32) * 0.125
        my = (geo_ref[i, 1, k : k + 1, :] - gy * PY).astype(F32) * 0.125
        ex.append((upper - mx).astype(BF))
        ey.append((py - my).astype(BF))
        oc = geo_ref[i, 2, k : k + 1, :]
        w = wt_ref[i, k : k + 1, :].astype(F32)
        levels = []
        for d in range(LV):
            cw = jnp.zeros((1, TR), F32)
            for o in range(NOC):
                cw = jnp.where(oc == o, cw_ref[o + d], cw)
            levels.append(jnp.broadcast_to(w * cw, (16, TR)).astype(BF))
        wd.append(levels)
    zero16 = jnp.zeros((16, TR), BF)

    def live_of(b, dx, kind):
        i, k = b // 2, b % 2
        base = (dx + 1) * 3
        if kind == 0:
            return ap_ref[i, k, base + 1]
        up = ap_ref[i, k, base + 2]
        down = ap_ref[i, k, base]
        return jnp.where(core == 1, up, down) if kind == 1 else jnp.where(core == 1, down, up)

    def amplitude(slot, dx, kind, nlev):
        shift = {0: 0, 1: step, 2: -step}[kind]
        for b in range(NB):
            gone = (1 - live_of(b, dx, kind)).astype(F32) * 64.0
            dy = jnp.abs(ey[b] + shift.astype(F32).astype(BF) if kind else ey[b]) + gone.astype(BF)
            for g in range(PX // 2):
                dist = jnp.abs(ex[b] + jnp.asarray(2 * dx + 0.25 * g, BF)) + dy
                level = jnp.floor(dist)
                for d in range(nlev):
                    a_ref[slot, 16 * g : 16 * g + 16, d * NJ + b * TR : d * NJ + b * TR + TR] = jnp.where(
                        level == d, wd[b][d], zero16
                    )

    def nlev_of(dx, kind):
        if kind == 0:
            return L_X if dx else L_OWN
        return LV if dx else L_Y

    for k in range(3):
        amplitude(k, *order[k], nlev_of(*order[k]))

    loads[5].wait()
    traces = tr_ref[...]
    for c in range(NC):
        t_ref[c] = jnp.dot(traces, i_ref[c], preferred_element_type=F32).astype(BF)

    for b in range(NB):
        i, k = b // 2, b % 2
        oc_row = jnp.broadcast_to(geo_ref[i, 2, k : k + 1, :], (TR, TR)).astype(F32)
        oc = jnp.transpose(oc_row)
        oc = jnp.concatenate([oc, oc], axis=1).astype(BF)
        for r in range(0, TR, 16):
            o = oc[r : r + 16]
            row = b * TR + r
            b2 = o >= 4
            o = jnp.where(b2, o - 4, o)
            b1 = o >= 2
            o = jnp.where(b1, o - 2, o)
            b0 = o >= 1
            t = [t_ref[c, row : row + 16, :] for c in range(NC)]
            t = [jnp.where(b2, t[c + 4], t[c]) for c in range(NC - 4)]
            t = [jnp.where(b1, t[c + 2], t[c]) for c in range(NC - 6)]
            t = [jnp.where(b0, t[c + 1], t[c]) for c in range(NC - 7)]
            for d in range(LV):
                v_ref[d * NJ + row : d * NJ + row + 16, :] = t[d]

    def migrate(slot, nlev):
        return jnp.dot(a_ref[slot, :, : nlev * NJ], v_ref[: nlev * NJ, :], preferred_element_type=F32)

    for k, n in enumerate(order):
        nlev = nlev_of(*n)
        if k >= 3:
            amplitude(k, *n, nlev)
        sent[k] = migrate(k, nlev).astype(BF)
        if k == 0:
            pl.semaphore_wait(barrier, count)
        guarded(exists(*n), lambda k=k: copies[k].start())

    amplitude(8, 0, 0, L_OWN)
    out_ref[...] = migrate(8, L_OWN).reshape(PX, PY, NT)

    for k in (7, 3, 4, 5, 6, 1, 2, 0):
        dx, kind = order[k]

        def take(k=k):
            copies[k].wait_recv()
            out_ref[...] += got[k].astype(F32).reshape(PX, PY, NT)

        guarded(exists(-dx, kind), take)

    for k, n in enumerate(order):
        guarded(exists(*n), lambda k=k: copies[k].wait_send())


def per_device(traces, aperture, geometry, trace_weight, class_weight, traveltime):
    hbm = pl.BlockSpec(memory_space=pltpu.HBM)
    tile = (PTS, NT)
    return pl.pallas_call(
        kernel,
        out_shape=jax.ShapeDtypeStruct((PX, PY, NT), F32),
        in_specs=[hbm] * 6,
        out_specs=pl.BlockSpec(memory_space=pltpu.VMEM),
        scratch_shapes=[
            pltpu.VMEM((NJ, NS), BF),
            pltpu.SMEM((2, 2, 9), jnp.int32),
            pltpu.VMEM((2, 3, 2, TR), jnp.int32),
            pltpu.VMEM((2, 2, TR), BF),
            pltpu.SMEM((NC,), F32),
            pltpu.VMEM((NC, NT), jnp.int32),
            pltpu.VMEM((NC, NS, NT), BF),
            pltpu.VMEM((NC, NJ, NT), BF),
            pltpu.VMEM((LV * NJ, NT), BF),
            pltpu.VMEM((9, PTS, LV * NJ), BF),
            pltpu.VMEM((8,) + tile, BF),
            pltpu.VMEM((8,) + tile, BF),
            pltpu.SemaphoreType.DMA((6,)),
            pltpu.SemaphoreType.DMA((8,)),
            pltpu.SemaphoreType.DMA((8,)),
        ],
        compiler_params=pltpu.CompilerParams(
            collective_id=0, has_side_effects=True, vmem_limit_bytes=32 * 1024 * 1024
        ),
        cost_estimate=pl.CostEstimate(flops=3_000_000_000, bytes_accessed=2_000_000, transcendentals=0),
        name="migrate",
    )(
        *(
            pltpu.with_memory_space_constraint(x, pltpu.HBM)
            for x in (
                traces.reshape(NJ, NS),
                aperture,
                geometry.transpose(0, 2, 1, 3),
                trace_weight,
                class_weight,
                traveltime,
            )
        )
    )


def solution(mesh):
    return jax.shard_map(
        per_device,
        mesh=mesh,
        in_specs=(
            P("gx", "gy", None, None),
            P("gx", "gy", None),
            P("gx", "gy", None, None),
            P("gx", "gy", None),
            P(),
            P(),
        ),
        out_specs=P("gx", "gy", None),
        check_vma=False,
    )
```

```python
import jax
import jax.numpy as jnp
from jax import lax
from jax.experimental import pallas as pl
from jax.experimental.pallas import tpu as pltpu
from jax.sharding import PartitionSpec as P

NS = 256
NT = 256
TR = 128
NB = 4
NJ = NB * TR
NC = 14
NOC = 8
PX = 16
PY = 8
PTS = PX * PY
L_OWN, L_X, L_Y, L_XY = 3, 5, 4, 6
LV = 7
MESH = pl.DeviceIdType.MESH
BF = jnp.bfloat16
F32 = jnp.float32


def kernel(
    tr_hbm, ap_hbm, geo_hbm, wt_hbm, cw_hbm, tt_hbm, out_ref,
    tr_ref, ap_ref, geo_ref, wt_ref, cw_ref, tt_ref, i_ref, t_ref, v_ref, a_ref, held, sent, got, load, send, recv,
):
    gx = lax.axis_index("gx")
    gy = lax.axis_index("gy")
    ngx = lax.axis_size("gx")
    ngy = lax.axis_size("gy")
    core = lax.rem(gy, 2)
    step = 2 * core - 1
    has_x = {-1: gx > 0, 1: gx < ngx - 1, 0: None}
    has_far = jnp.logical_and(gy + step >= 0, gy + step < ngy)
    column = gy // 2
    rank = lax.rem(column, 4)
    at_end = jnp.where(core == 1, rank == 3, rank == 0)
    route = jnp.logical_and(at_end, has_far)
    early = jnp.logical_or(jnp.logical_and(gx == 0, jnp.logical_and(route, lax.rem(column // 4, 2) == 0)), gx + gy == 1)

    order = [(0, 1), (-1, 1), (1, 1), (-1, 2), (1, 2), (0, 2), (-1, 0), (1, 0)]

    def device(dx, kind):
        return (gx + dx, gy + {0: 0, 1: step, 2: -step}[kind])

    def exists(dx, kind):
        side = has_x[dx]
        if kind == 1:
            return has_far if side is None else jnp.logical_and(side, has_far)
        return side

    def guarded(cond, body):
        if cond is None:
            body()
        else:
            pl.when(cond)(body)

    loads = [
        pltpu.make_async_copy(src, dst, load.at[k])
        for k, (src, dst) in enumerate(
            [(tt_hbm, tt_ref), (tr_hbm, tr_ref), (geo_hbm, geo_ref), (wt_hbm, wt_ref), (cw_hbm, cw_ref), (ap_hbm, ap_ref)]
        )
    ]
    loads[0].start()
    loads[1].start()

    barrier = pltpu.get_barrier_semaphore()
    count = jnp.int32(1)
    greeted = [(0, 1, has_far), (-1, 1, None), (1, 1, None), (-1, 0, has_x[-1]), (1, 0, has_x[1])]
    for dx, kind, cond in greeted:
        if cond is None:
            cond = jnp.logical_and(route, has_x[dx])
        pl.when(cond)(
            lambda dx=dx, kind=kind: pl.semaphore_signal(
                barrier, inc=1, device_id=device(dx, kind), device_id_type=MESH
            )
        )
        count = count + cond.astype(jnp.int32)
    pl.semaphore_signal(barrier, inc=1, device_id=device(0, 2), device_id_type=MESH)

    for copy in loads[2:]:
        copy.start()

    copies = []
    for k, (dx, kind) in enumerate(order):
        target = device(dx, kind)
        if dx and kind == 1:
            target = (jnp.where(at_end, gx + dx, gx), gy + step)
        elif dx and kind == 2:
            target = device(0, 2)
        copies.append(
            pltpu.make_async_remote_copy(
                src_ref=sent.at[k],
                dst_ref=got.at[k],
                send_sem=send.at[k],
                recv_sem=recv.at[k],
                device_id=target,
                device_id_type=MESH,
            )
        )

    loads[0].wait()
    sample = lax.broadcasted_iota(jnp.int32, (NS, NT), 0).astype(F32).astype(BF)
    zero = jnp.zeros((NS, NT), BF)
    for c in range(NC):
        q = tt_ref[c : c + 1, :]
        first = q // 4
        frac = (q % 4).astype(F32) * 0.25
        s0 = jnp.broadcast_to(first.astype(F32), (NS, NT)).astype(BF)
        s1 = jnp.broadcast_to((first + 1).astype(F32), (NS, NT)).astype(BF)
        w1 = jnp.broadcast_to(frac, (NS, NT)).astype(BF)
        w0 = jnp.broadcast_to(1.0 - frac, (NS, NT)).astype(BF)
        i_ref[c] = jnp.where(sample == s0, w0, jnp.where(sample == s1, w1, zero))

    for copy in loads[2:]:
        copy.wait()
    row16 = lax.broadcasted_iota(jnp.int32, (16, TR), 0)
    upper = (row16 // 8).astype(F32) * 0.125
    py = (row16 % 8).astype(F32) * 0.125
    ex, ey, wd = [], [], []
    for b in range(NB):
        i, k = b // 2, b % 2
        mx = (geo_ref[i, 0, k : k + 1, :] - gx * PX).astype(F32) * 0.125
        my = (geo_ref[i, 1, k : k + 1, :] - gy * PY).astype(F32) * 0.125
        ex.append((upper - mx).astype(BF))
        ey.append((py - my).astype(BF))
        oc = geo_ref[i, 2, k : k + 1, :]
        w = wt_ref[i, k : k + 1, :].astype(F32)
        levels = []
        for d in range(LV):
            cw = jnp.zeros((1, TR), F32)
            for o in range(NOC):
                cw = jnp.where(oc == o, cw_ref[o + d], cw)
            levels.append(jnp.broadcast_to(w * cw, (16, TR)).astype(BF))
        wd.append(levels)
    zero16 = jnp.zeros((16, TR), BF)

    def live_of(b, dx, kind):
        i, k = b // 2, b % 2
        base = (dx + 1) * 3
        if kind == 0:
            return ap_ref[i, k, base + 1]
        up = ap_ref[i, k, base + 2]
        down = ap_ref[i, k, base]
        return jnp.where(core == 1, up, down) if kind == 1 else jnp.where(core == 1, down, up)

    def amplitude(slot, dx, kind, nlev):
        shift = {0: 0, 1: step, 2: -step}[kind]
        for b in range(NB):
            gone = (1 - live_of(b, dx, kind)).astype(F32) * 64.0
            dy = jnp.abs(ey[b] + shift.astype(F32).astype(BF) if kind else ey[b]) + gone.astype(BF)
            for g in range(PX // 2):
                dist = jnp.abs(ex[b] + jnp.asarray(2 * dx + 0.25 * g, BF)) + dy
                level = jnp.floor(dist)
                for d in range(nlev):
                    a_ref[slot, 16 * g : 16 * g + 16, d * NJ + b * TR : d * NJ + b * TR + TR] = jnp.where(
                        level == d, wd[b][d], zero16
                    )

    def nlev_of(dx, kind):
        if kind == 0:
            return L_X if dx else L_OWN
        return LV if dx else L_Y

    loads[1].wait()
    columns = []
    for b in range(NB):
        i, k = b // 2, b % 2
        oc = jnp.transpose(jnp.broadcast_to(geo_ref[i, 2, k : k + 1, :], (TR, TR)).astype(F32))
        columns.append(jnp.concatenate([oc, oc], axis=1).astype(BF))

    def interpolate(c):
        t_ref[c] = jnp.dot(tr_ref[...], i_ref[c], preferred_element_type=F32).astype(BF)

    def pick(lo, hi):
        for b in range(NB):
            for r in range(0, TR, 16):
                o = columns[b][r : r + 16]
                row = b * TR + r
                b2 = o >= 4
                o = jnp.where(b2, o - 4, o)
                b1 = o >= 2
                o = jnp.where(b1, o - 2, o)
                b0 = o >= 1
                t = [t_ref[c, row : row + 16, :] for c in range(lo, hi + NOC - 1)]
                t = [jnp.where(b2, t[c + 4], t[c]) for c in range(len(t) - 4)]
                t = [jnp.where(b1, t[c + 2], t[c]) for c in range(len(t) - 2)]
                t = [jnp.where(b0, t[c + 1], t[c]) for c in range(len(t) - 1)]
                for d in range(lo, hi):
                    v_ref[d * NJ + row : d * NJ + row + 16, :] = t[d - lo]

    def migrate(slot, nlev):
        return jnp.dot(a_ref[slot, :, : nlev * NJ], v_ref[: nlev * NJ, :], preferred_element_type=F32)

    for c in range(L_Y + NOC - 1):
        interpolate(c)
    pick(0, L_Y)

    for k, n in enumerate(order):
        nlev = nlev_of(*n)
        if k == 1:
            for c in range(L_Y + NOC - 1, NC):
                interpolate(c)
            pick(L_Y, LV)

        def make(k=k, n=n, nlev=nlev):
            amplitude(k, *n, nlev)
            tile = migrate(k, nlev)
            if k < 6:
                sent[k] = tile.astype(BF)
            else:
                held[k - 6] = tile

        guarded(exists(*n), make)
        if k < 6:

            @pl.when(jnp.logical_not(early))
            def _(k=k, n=n):
                if k == 0:
                    pl.semaphore_wait(barrier, count)
                guarded(exists(*n), lambda: copies[k].start())

    amplitude(8, 0, 0, L_OWN)
    out_ref[...] = migrate(8, L_OWN).reshape(PX, PY, NT)

    @pl.when(early)
    def _():
        pl.semaphore_wait(barrier, count)
        for k, n in enumerate(order[:6]):
            guarded(exists(*n), lambda k=k: copies[k].start())

    def add(k):
        copies[k].wait_recv()
        out_ref[...] += got[k].astype(F32).reshape(PX, PY, NT)

    add(5)

    for dx, corner, near, k in ((-1, 1, 3, 6), (1, 2, 4, 7)):

        @pl.when(has_x[dx])
        def _(corner=corner, near=near, k=k):
            copies[near].wait_recv()
            held[k - 6] += got[near].astype(F32)

            @pl.when(jnp.logical_and(has_far, jnp.logical_not(at_end)))
            def _():
                copies[corner].wait_recv()
                held[k - 6] += got[corner].astype(F32)

            sent[k] = held[k - 6].astype(BF)
            copies[k].start()

    pl.when(jnp.logical_and(has_far, jnp.logical_not(at_end)))(lambda: add(0))
    pl.when(has_x[1])(lambda: add(6))
    pl.when(has_x[-1])(lambda: add(7))

    @pl.when(route)
    def _():
        add(0)
        pl.when(has_x[1])(lambda: add(1))
        pl.when(has_x[-1])(lambda: add(2))

    for k, n in enumerate(order):
        guarded(exists(*n), lambda k=k: copies[k].wait_send())


def per_device(traces, aperture, geometry, trace_weight, class_weight, traveltime):
    hbm = pl.BlockSpec(memory_space=pltpu.HBM)
    tile = (PTS, NT)
    return pl.pallas_call(
        kernel,
        out_shape=jax.ShapeDtypeStruct((PX, PY, NT), F32),
        in_specs=[hbm] * 6,
        out_specs=pl.BlockSpec(memory_space=pltpu.VMEM),
        scratch_shapes=[
            pltpu.VMEM((NJ, NS), BF),
            pltpu.SMEM((2, 2, 9), jnp.int32),
            pltpu.VMEM((2, 3, 2, TR), jnp.int32),
            pltpu.VMEM((2, 2, TR), BF),
            pltpu.SMEM((NC,), F32),
            pltpu.VMEM((NC, NT), jnp.int32),
            pltpu.VMEM((NC, NS, NT), BF),
            pltpu.VMEM((NC, NJ, NT), BF),
            pltpu.VMEM((LV * NJ, NT), BF),
            pltpu.VMEM((9, PTS, LV * NJ), BF),
            pltpu.VMEM((2,) + tile, F32),
            pltpu.VMEM((8,) + tile, BF),
            pltpu.VMEM((8,) + tile, BF),
            pltpu.SemaphoreType.DMA((6,)),
            pltpu.SemaphoreType.DMA((8,)),
            pltpu.SemaphoreType.DMA((8,)),
        ],
        compiler_params=pltpu.CompilerParams(
            collective_id=0, has_side_effects=True, vmem_limit_bytes=32 * 1024 * 1024
        ),
        cost_estimate=pl.CostEstimate(flops=3_000_000_000, bytes_accessed=2_000_000, transcendentals=0),
        name="migrate",
    )(
        *(
            pltpu.with_memory_space_constraint(x, pltpu.HBM)
            for x in (
                traces.reshape(NJ, NS),
                aperture,
                geometry.transpose(0, 2, 1, 3),
                trace_weight,
                class_weight,
                traveltime,
            )
        )
    )


def solution(mesh):
    return jax.shard_map(
        per_device,
        mesh=mesh,
        in_specs=(
            P("gx", "gy", None, None),
            P("gx", "gy", None),
            P("gx", "gy", None, None),
            P("gx", "gy", None),
            P(),
            P(),
        ),
        out_specs=P("gx", "gy", None),
        check_vma=False,
    )
```

```python
import jax
import jax.numpy as jnp
from jax import lax
from jax.experimental import pallas as pl
from jax.experimental.pallas import tpu as pltpu
from jax.sharding import PartitionSpec as P

NS = 256
NT = 256
TR = 128
NB = 4
NJ = NB * TR
NC = 14
NOC = 8
PX = 16
PY = 8
PTS = PX * PY
L_OWN, L_X, L_Y, L_XY = 3, 5, 4, 6
LV = 7
MESH = pl.DeviceIdType.MESH
BF = jnp.bfloat16
F32 = jnp.float32


def kernel(
    tr_hbm, ap_hbm, geo_hbm, wt_hbm, cw_hbm, tt_hbm, out_ref,
    tr_ref, ap_ref, geo_ref, wt_ref, cw_ref, tt_ref, i_ref, t_ref, v_ref, a_ref, held, sent, got, load, send, recv, near_sem,
):
    gx = lax.axis_index("gx")
    gy = lax.axis_index("gy")
    ngx = lax.axis_size("gx")
    ngy = lax.axis_size("gy")
    core = lax.rem(gy, 2)
    step = 2 * core - 1
    has_x = {-1: gx > 0, 1: gx < ngx - 1, 0: None}
    has_far = jnp.logical_and(gy + step >= 0, gy + step < ngy)
    column = gy // 2
    rank = lax.rem(column, 4)
    at_end = jnp.where(core == 1, rank == 3, rank == 0)
    route = jnp.logical_and(at_end, has_far)
    near_half = lax.rem(column // 4, 2) == 0
    partner_at_end = jnp.where(core == 1, rank == 0, rank == 3)
    partner_far = gy - 2 * step
    beside_route = jnp.logical_and(partner_at_end, jnp.logical_and(partner_far >= 0, partner_far < ngy))
    bend = column // 8 == 3
    late = jnp.logical_and(route, jnp.logical_and(near_half, gx == 0))
    inner = jnp.logical_and(route, jnp.logical_and(near_half, gx == 1))
    early = gx + gy == 1
    quick = jnp.logical_and(jnp.logical_not(early), jnp.logical_or(jnp.logical_not(route), jnp.logical_and(jnp.logical_and(gx < 2, jnp.logical_not(bend)), jnp.logical_not(near_half))))
    middle = jnp.logical_and(route, jnp.logical_not(jnp.logical_or(inner, jnp.logical_or(quick, late))))
    origin = gx + gy == 0
    beside = jnp.logical_and(gx == 0, gy == 1)
    across = jnp.logical_and(gx == 1, gy == 1)

    order = [(0, 1), (-1, 1), (1, 1), (-1, 2), (1, 2), (0, 2), (-1, 0), (1, 0)]

    def device(dx, kind):
        return (gx + dx, gy + {0: 0, 1: step, 2: -step}[kind])

    def exists(dx, kind):
        side = has_x[dx]
        if kind == 1:
            return has_far if side is None else jnp.logical_and(side, has_far)
        return side

    def guarded(cond, body):
        if cond is None:
            body()
        else:
            pl.when(cond)(body)

    loads = [
        pltpu.make_async_copy(src, dst, load.at[k])
        for k, (src, dst) in enumerate(
            [(tt_hbm, tt_ref), (tr_hbm, tr_ref), (geo_hbm, geo_ref), (wt_hbm, wt_ref), (cw_hbm, cw_ref), (ap_hbm, ap_ref)]
        )
    ]
    loads[0].start()
    loads[1].start()

    barrier = pltpu.get_barrier_semaphore()
    off_route = jnp.logical_not(route)

    def greet(cond, dx, kind):
        pl.when(cond)(
            lambda: pl.semaphore_signal(barrier, inc=1, device_id=device(dx, kind), device_id_type=MESH)
        )

    greet(has_far, 0, 1)
    for dx in (-1, 1):
        greet(jnp.logical_and(route, has_x[dx]), dx, 1)
        greet(jnp.logical_and(off_route, has_x[dx]), dx, 0)
        greet(jnp.logical_and(route, has_x[dx]), dx, 2)
    greet(jnp.logical_not(beside_route), 0, 2)
    sides = has_x[-1].astype(jnp.int32) + has_x[1].astype(jnp.int32)
    count = jnp.where(
        route, 1 + sides, 1 + has_far.astype(jnp.int32) + sides + jnp.where(beside_route, sides, 0)
    )
    pl.when(across)(
        lambda: pl.semaphore_signal(barrier, inc=1, device_id=(gx - 1, gy - 1), device_id_type=MESH)
    )
    count = count + origin.astype(jnp.int32)

    for copy in loads[2:]:
        copy.start()

    copies = []
    for k, (dx, kind) in enumerate(order):
        target = device(dx, kind)
        if dx and kind == 1:
            target = (jnp.where(at_end, gx + dx, gx), gy + step)
        elif dx and kind == 2:
            target = device(0, 2)
        copies.append(
            pltpu.make_async_remote_copy(
                src_ref=sent.at[k],
                dst_ref=got.at[k],
                send_sem=send.at[k],
                recv_sem=recv.at[k],
                device_id=target,
                device_id_type=MESH,
            )
        )

    copies.append(
        pltpu.make_async_remote_copy(
            src_ref=sent.at[4],
            dst_ref=got.at[8],
            send_sem=send.at[8],
            recv_sem=recv.at[8],
            device_id=(gx + 1, gy + 1),
            device_id_type=MESH,
        )
    )

    loads[0].wait()
    sample = lax.broadcasted_iota(jnp.int32, (NS, NT), 0).astype(F32).astype(BF)
    zero = jnp.zeros((NS, NT), BF)
    for c in range(NC):
        q = tt_ref[c : c + 1, :]
        first = q // 4
        frac = (q % 4).astype(F32) * 0.25
        s0 = jnp.broadcast_to(first.astype(F32), (NS, NT)).astype(BF)
        s1 = jnp.broadcast_to((first + 1).astype(F32), (NS, NT)).astype(BF)
        w1 = jnp.broadcast_to(frac, (NS, NT)).astype(BF)
        w0 = jnp.broadcast_to(1.0 - frac, (NS, NT)).astype(BF)
        i_ref[c] = jnp.where(sample == s0, w0, jnp.where(sample == s1, w1, zero))

    for copy in loads[2:]:
        copy.wait()
    row16 = lax.broadcasted_iota(jnp.int32, (16, TR), 0)
    upper = (row16 // 8).astype(F32) * 0.125
    py = (row16 % 8).astype(F32) * 0.125
    ex, ey, wd = [], [], []
    for b in range(NB):
        i, k = b // 2, b % 2
        mx = (geo_ref[i, 0, k : k + 1, :] - gx * PX).astype(F32) * 0.125
        my = (geo_ref[i, 1, k : k + 1, :] - gy * PY).astype(F32) * 0.125
        ex.append((upper - mx).astype(BF))
        ey.append((py - my).astype(BF))
        oc = geo_ref[i, 2, k : k + 1, :]
        w = wt_ref[i, k : k + 1, :].astype(F32)
        levels = []
        for d in range(LV):
            cw = jnp.zeros((1, TR), F32)
            for o in range(NOC):
                cw = jnp.where(oc == o, cw_ref[o + d], cw)
            levels.append(jnp.broadcast_to(w * cw, (16, TR)).astype(BF))
        wd.append(levels)
    zero16 = jnp.zeros((16, TR), BF)

    def live_of(b, dx, kind):
        i, k = b // 2, b % 2
        base = (dx + 1) * 3
        if kind == 0:
            return ap_ref[i, k, base + 1]
        up = ap_ref[i, k, base + 2]
        down = ap_ref[i, k, base]
        return jnp.where(core == 1, up, down) if kind == 1 else jnp.where(core == 1, down, up)

    def amplitude(slot, dx, kind, nlev):
        shift = {0: 0, 1: step, 2: -step}[kind]
        for b in range(NB):
            gone = (1 - live_of(b, dx, kind)).astype(F32) * 64.0
            dy = jnp.abs(ey[b] + shift.astype(F32).astype(BF) if kind else ey[b]) + gone.astype(BF)
            for g in range(PX // 2):
                dist = jnp.abs(ex[b] + jnp.asarray(2 * dx + 0.25 * g, BF)) + dy
                level = jnp.floor(dist)
                for d in range(nlev):
                    a_ref[slot, 16 * g : 16 * g + 16, d * NJ + b * TR : d * NJ + b * TR + TR] = jnp.where(
                        level == d, wd[b][d], zero16
                    )

    def nlev_of(dx, kind):
        if kind == 0:
            return L_X if dx else L_OWN
        return LV if dx else L_Y

    loads[1].wait()
    columns = []
    for b in range(NB):
        i, k = b // 2, b % 2
        oc = jnp.transpose(jnp.broadcast_to(geo_ref[i, 2, k : k + 1, :], (TR, TR)).astype(F32))
        columns.append(jnp.concatenate([oc, oc], axis=1).astype(BF))

    def interpolate(c):
        t_ref[c] = jnp.dot(tr_ref[...], i_ref[c], preferred_element_type=F32).astype(BF)

    def pick(lo, hi):
        for b in range(NB):
            for r in range(0, TR, 16):
                o = columns[b][r : r + 16]
                row = b * TR + r
                b2 = o >= 4
                o = jnp.where(b2, o - 4, o)
                b1 = o >= 2
                o = jnp.where(b1, o - 2, o)
                b0 = o >= 1
                t = [t_ref[c, row : row + 16, :] for c in range(lo, hi + NOC - 1)]
                t = [jnp.where(b2, t[c + 4], t[c]) for c in range(len(t) - 4)]
                t = [jnp.where(b1, t[c + 2], t[c]) for c in range(len(t) - 2)]
                t = [jnp.where(b0, t[c + 1], t[c]) for c in range(len(t) - 1)]
                for d in range(lo, hi):
                    v_ref[d * NJ + row : d * NJ + row + 16, :] = t[d - lo]

    def migrate(slot, nlev):
        return jnp.dot(a_ref[slot, :, : nlev * NJ], v_ref[: nlev * NJ, :], preferred_element_type=F32)

    for c in range(L_Y + NOC - 1):
        interpolate(c)
    pick(0, L_Y)

    def make(k):
        dx, kind = order[k]
        nlev = nlev_of(dx, kind)

        def body():
            amplitude(k, dx, kind, nlev)
            tile = migrate(k, nlev)
            if k < 6:
                sent[k] = tile.astype(BF)
            else:
                held[k - 6] = tile

        guarded(exists(dx, kind), body)

    def start(*slots):
        for k in slots:
            cond = exists(*order[k])
            if k == 4:
                pl.when(origin)(lambda: copies[8].start())
                cond = jnp.logical_and(cond, jnp.logical_not(origin))
            guarded(cond, lambda k=k: copies[k].start())

    def own():
        amplitude(8, 0, 0, L_OWN)
        out_ref[...] = migrate(8, L_OWN).reshape(PX, PY, NT)

    def meet():
        pl.semaphore_wait(barrier, count)
        pl.when(beside_route)(
            lambda: pl.semaphore_signal(near_sem, inc=1, device_id=device(0, 2), device_id_type=MESH)
        )

    make(0)

    @pl.when(quick)
    def _():
        meet()
        start(0)

    for c in range(L_Y + NOC - 1, NC):
        interpolate(c)
    pick(L_Y, LV)
    make(1)
    make(2)

    def start_far():
        low = gx < 2
        pl.when(low)(lambda: start(2))
        pl.when(jnp.logical_not(low))(lambda: start(1))
        start(0)
        pl.when(low)(lambda: start(1))
        pl.when(jnp.logical_not(low))(lambda: start(2))

    @pl.when(middle)
    def _():
        meet()
        start_far()

    pl.when(quick)(lambda: start(1, 2))
    make(3)
    make(4)
    make(5)
    pl.when(route)(lambda: pl.semaphore_wait(near_sem, 1))
    pl.when(jnp.logical_not(early))(lambda: start(3, 4, 5))
    make(6)
    make(7)

    @pl.when(inner)
    def _():
        meet()
        start_far()

    @pl.when(early)
    def _():
        own()
        meet()
        start(0, 1, 2, 3, 4, 5)

    off_far = jnp.logical_and(has_far, jnp.logical_not(at_end))

    for dx, corner, near, k in ((-1, 1, 3, 6), (1, 2, 4, 7)):

        @pl.when(has_x[dx])
        def _(corner=corner, near=near, k=k):
            @pl.when(jnp.logical_not(beside))
            def _():
                copies[near].wait_recv()
                held[k - 6] += got[near].astype(F32)

            @pl.when(off_far)
            def _():
                copies[corner].wait_recv()
                held[k - 6] += got[corner].astype(F32)

            sent[k] = held[k - 6].astype(BF)
            copies[k].start()

    pl.when(jnp.logical_not(early))(own)

    @pl.when(late)
    def _():
        meet()
        start_far()

    def add(k):
        copies[k].wait_recv()
        out_ref[...] += got[k].astype(F32).reshape(PX, PY, NT)

    add(5)
    pl.when(off_far)(lambda: add(0))
    pl.when(has_x[1])(lambda: add(6))
    pl.when(has_x[-1])(lambda: add(7))
    pl.when(across)(lambda: add(8))

    @pl.when(route)
    def _():
        add(0)
        pl.when(has_x[1])(lambda: add(1))
        pl.when(has_x[-1])(lambda: add(2))

    for k, n in enumerate(order):
        cond = exists(*n)
        if k == 4:
            pl.when(origin)(lambda: copies[8].wait_send())
            cond = jnp.logical_and(cond, jnp.logical_not(origin))
        guarded(cond, lambda k=k: copies[k].wait_send())


def per_device(traces, aperture, geometry, trace_weight, class_weight, traveltime):
    hbm = pl.BlockSpec(memory_space=pltpu.HBM)
    tile = (PTS, NT)
    return pl.pallas_call(
        kernel,
        out_shape=jax.ShapeDtypeStruct((PX, PY, NT), F32),
        in_specs=[hbm] * 6,
        out_specs=pl.BlockSpec(memory_space=pltpu.VMEM),
        scratch_shapes=[
            pltpu.VMEM((NJ, NS), BF),
            pltpu.SMEM((2, 2, 9), jnp.int32),
            pltpu.VMEM((2, 3, 2, TR), jnp.int32),
            pltpu.VMEM((2, 2, TR), BF),
            pltpu.SMEM((NC,), F32),
            pltpu.VMEM((NC, NT), jnp.int32),
            pltpu.VMEM((NC, NS, NT), BF),
            pltpu.VMEM((NC, NJ, NT), BF),
            pltpu.VMEM((LV * NJ, NT), BF),
            pltpu.VMEM((9, PTS, LV * NJ), BF),
            pltpu.VMEM((2,) + tile, F32),
            pltpu.VMEM((8,) + tile, BF),
            pltpu.VMEM((9,) + tile, BF),
            pltpu.SemaphoreType.DMA((6,)),
            pltpu.SemaphoreType.DMA((9,)),
            pltpu.SemaphoreType.DMA((9,)),
            pltpu.SemaphoreType.REGULAR,
        ],
        compiler_params=pltpu.CompilerParams(
            collective_id=0, has_side_effects=True, vmem_limit_bytes=32 * 1024 * 1024
        ),
        cost_estimate=pl.CostEstimate(flops=3_000_000_000, bytes_accessed=2_000_000, transcendentals=0),
        name="migrate",
    )(
        *(
            pltpu.with_memory_space_constraint(x, pltpu.HBM)
            for x in (
                traces.reshape(NJ, NS),
                aperture,
                geometry.transpose(0, 2, 1, 3),
                trace_weight,
                class_weight,
                traveltime,
            )
        )
    )


def solution(mesh):
    return jax.shard_map(
        per_device,
        mesh=mesh,
        in_specs=(
            P("gx", "gy", None, None),
            P("gx", "gy", None),
            P("gx", "gy", None, None),
            P("gx", "gy", None),
            P(),
            P(),
        ),
        out_specs=P("gx", "gy", None),
        check_vma=False,
    )
```

```python
import jax
import jax.numpy as jnp
from jax import lax
from jax.experimental import pallas as pl
from jax.experimental.pallas import tpu as pltpu
from jax.sharding import PartitionSpec as P

NS = 256
NT = 256
TR = 128
NB = 4
NJ = NB * TR
NC = 14
NOC = 8
PX = 16
PY = 8
PTS = PX * PY
L_OWN, L_X, L_Y, L_XY = 3, 5, 4, 6
LV = 7
MESH = pl.DeviceIdType.MESH
BF = jnp.bfloat16
F32 = jnp.float32


def kernel(
    tr_hbm, ap_hbm, geo_hbm, wt_hbm, cw_hbm, tt_hbm, out_ref,
    tr_ref, ap_ref, geo_ref, wt_ref, cw_ref, tt_ref, i_ref, t_ref, v_ref, a_ref, held, sent, got, load, send, recv, near_sem,
):
    gx = lax.axis_index("gx")
    gy = lax.axis_index("gy")
    ngx = lax.axis_size("gx")
    ngy = lax.axis_size("gy")
    core = lax.rem(gy, 2)
    step = 2 * core - 1
    has_x = {-1: gx > 0, 1: gx < ngx - 1, 0: None}
    has_far = jnp.logical_and(gy + step >= 0, gy + step < ngy)
    column = gy // 2
    rank = lax.rem(column, 4)
    at_end = jnp.where(core == 1, rank == 3, rank == 0)
    route = jnp.logical_and(at_end, has_far)
    near_half = lax.rem(column // 4, 2) == 0
    partner_at_end = jnp.where(core == 1, rank == 0, rank == 3)
    partner_far = gy - 2 * step
    beside_route = jnp.logical_and(partner_at_end, jnp.logical_and(partner_far >= 0, partner_far < ngy))
    bend = column // 8 == 3
    late = jnp.logical_and(route, jnp.logical_and(near_half, gx == 0))
    inner = gx < 0
    early = gx + gy == 1
    quick = jnp.logical_and(jnp.logical_not(early), jnp.logical_not(late))
    middle = jnp.logical_and(route, jnp.logical_not(jnp.logical_or(inner, jnp.logical_or(quick, late))))
    origin = gx + gy == 0
    beside = jnp.logical_and(gx == 0, gy == 1)
    across = jnp.logical_and(gx == 1, gy == 1)

    order = [(0, 1), (-1, 1), (1, 1), (-1, 2), (1, 2), (0, 2), (-1, 0), (1, 0)]

    def device(dx, kind):
        return (gx + dx, gy + {0: 0, 1: step, 2: -step}[kind])

    def exists(dx, kind):
        side = has_x[dx]
        if kind == 1:
            return has_far if side is None else jnp.logical_and(side, has_far)
        return side

    def guarded(cond, body):
        if cond is None:
            body()
        else:
            pl.when(cond)(body)

    loads = [
        pltpu.make_async_copy(src, dst, load.at[k])
        for k, (src, dst) in enumerate(
            [(tt_hbm, tt_ref), (tr_hbm, tr_ref), (geo_hbm, geo_ref), (wt_hbm, wt_ref), (cw_hbm, cw_ref), (ap_hbm, ap_ref)]
        )
    ]
    loads[0].start()
    loads[1].start()

    barrier = pltpu.get_barrier_semaphore()
    off_route = jnp.logical_not(route)

    def greet(cond, dx, kind):
        pl.when(cond)(
            lambda: pl.semaphore_signal(barrier, inc=1, device_id=device(dx, kind), device_id_type=MESH)
        )

    greet(has_far, 0, 1)
    for dx in (-1, 1):
        greet(jnp.logical_and(route, has_x[dx]), dx, 1)
        greet(jnp.logical_and(off_route, has_x[dx]), dx, 0)
        greet(jnp.logical_and(route, has_x[dx]), dx, 2)
    greet(jnp.logical_not(beside_route), 0, 2)
    sides = has_x[-1].astype(jnp.int32) + has_x[1].astype(jnp.int32)
    count = jnp.where(
        route, 1 + sides, 1 + has_far.astype(jnp.int32) + sides + jnp.where(beside_route, sides, 0)
    )
    pl.when(across)(
        lambda: pl.semaphore_signal(barrier, inc=1, device_id=(gx - 1, gy - 1), device_id_type=MESH)
    )
    count = count + origin.astype(jnp.int32)

    for copy in loads[2:]:
        copy.start()

    copies = []
    for k, (dx, kind) in enumerate(order):
        target = device(dx, kind)
        if dx and kind == 1:
            target = (jnp.where(at_end, gx + dx, gx), gy + step)
        elif dx and kind == 2:
            target = device(0, 2)
        copies.append(
            pltpu.make_async_remote_copy(
                src_ref=sent.at[k],
                dst_ref=got.at[k],
                send_sem=send.at[k],
                recv_sem=recv.at[k],
                device_id=target,
                device_id_type=MESH,
            )
        )

    copies.append(
        pltpu.make_async_remote_copy(
            src_ref=sent.at[4],
            dst_ref=got.at[8],
            send_sem=send.at[8],
            recv_sem=recv.at[8],
            device_id=(gx + 1, gy + 1),
            device_id_type=MESH,
        )
    )

    loads[0].wait()
    sample = lax.broadcasted_iota(jnp.int32, (NS, NT), 0).astype(F32).astype(BF)
    zero = jnp.zeros((NS, NT), BF)
    for c in range(NC):
        q = tt_ref[c : c + 1, :]
        first = q // 4
        frac = (q % 4).astype(F32) * 0.25
        s0 = jnp.broadcast_to(first.astype(F32), (NS, NT)).astype(BF)
        s1 = jnp.broadcast_to((first + 1).astype(F32), (NS, NT)).astype(BF)
        w1 = jnp.broadcast_to(frac, (NS, NT)).astype(BF)
        w0 = jnp.broadcast_to(1.0 - frac, (NS, NT)).astype(BF)
        i_ref[c] = jnp.where(sample == s0, w0, jnp.where(sample == s1, w1, zero))

    for copy in loads[2:]:
        copy.wait()
    row16 = lax.broadcasted_iota(jnp.int32, (16, TR), 0)
    upper = (row16 // 8).astype(F32) * 0.125
    py = (row16 % 8).astype(F32) * 0.125
    ex, ey, wd = [], [], []
    for b in range(NB):
        i, k = b // 2, b % 2
        mx = (geo_ref[i, 0, k : k + 1, :] - gx * PX).astype(F32) * 0.125
        my = (geo_ref[i, 1, k : k + 1, :] - gy * PY).astype(F32) * 0.125
        ex.append((upper - mx).astype(BF))
        ey.append((py - my).astype(BF))
        oc = geo_ref[i, 2, k : k + 1, :]
        w = wt_ref[i, k : k + 1, :].astype(F32)
        levels = []
        for d in range(LV):
            cw = jnp.zeros((1, TR), F32)
            for o in range(NOC):
                cw = jnp.where(oc == o, cw_ref[o + d], cw)
            levels.append(jnp.broadcast_to(w * cw, (16, TR)).astype(BF))
        wd.append(levels)
    zero16 = jnp.zeros((16, TR), BF)

    def live_of(b, dx, kind):
        i, k = b // 2, b % 2
        base = (dx + 1) * 3
        if kind == 0:
            return ap_ref[i, k, base + 1]
        up = ap_ref[i, k, base + 2]
        down = ap_ref[i, k, base]
        return jnp.where(core == 1, up, down) if kind == 1 else jnp.where(core == 1, down, up)

    def amplitude(slot, dx, kind, nlev):
        shift = {0: 0, 1: step, 2: -step}[kind]
        for b in range(NB):
            gone = (1 - live_of(b, dx, kind)).astype(F32) * 64.0
            dy = jnp.abs(ey[b] + shift.astype(F32).astype(BF) if kind else ey[b]) + gone.astype(BF)
            for g in range(PX // 2):
                dist = jnp.abs(ex[b] + jnp.asarray(2 * dx + 0.25 * g, BF)) + dy
                level = jnp.floor(dist)
                for d in range(nlev):
                    a_ref[slot, 16 * g : 16 * g + 16, d * NJ + b * TR : d * NJ + b * TR + TR] = jnp.where(
                        level == d, wd[b][d], zero16
                    )

    def nlev_of(dx, kind):
        if kind == 0:
            return L_X if dx else L_OWN
        return LV if dx else L_Y

    loads[1].wait()
    columns = []
    for b in range(NB):
        i, k = b // 2, b % 2
        oc = jnp.transpose(jnp.broadcast_to(geo_ref[i, 2, k : k + 1, :], (TR, TR)).astype(F32))
        columns.append(jnp.concatenate([oc, oc], axis=1).astype(BF))

    def interpolate(c):
        t_ref[c] = jnp.dot(tr_ref[...], i_ref[c], preferred_element_type=F32).astype(BF)

    def pick(lo, hi):
        for b in range(NB):
            for r in range(0, TR, 16):
                o = columns[b][r : r + 16]
                row = b * TR + r
                b2 = o >= 4
                o = jnp.where(b2, o - 4, o)
                b1 = o >= 2
                o = jnp.where(b1, o - 2, o)
                b0 = o >= 1
                t = [t_ref[c, row : row + 16, :] for c in range(lo, hi + NOC - 1)]
                t = [jnp.where(b2, t[c + 4], t[c]) for c in range(len(t) - 4)]
                t = [jnp.where(b1, t[c + 2], t[c]) for c in range(len(t) - 2)]
                t = [jnp.where(b0, t[c + 1], t[c]) for c in range(len(t) - 1)]
                for d in range(lo, hi):
                    v_ref[d * NJ + row : d * NJ + row + 16, :] = t[d - lo]

    def migrate(slot, nlev):
        return jnp.dot(a_ref[slot, :, : nlev * NJ], v_ref[: nlev * NJ, :], preferred_element_type=F32)

    for c in range(L_Y + NOC - 1):
        interpolate(c)
    pick(0, L_Y)

    def make(k):
        dx, kind = order[k]
        nlev = nlev_of(dx, kind)

        def body():
            amplitude(k, dx, kind, nlev)
            tile = migrate(k, nlev)
            if k < 6:
                sent[k] = tile.astype(BF)
            else:
                held[k - 6] = tile

        guarded(exists(dx, kind), body)

    def start(*slots):
        for k in slots:
            cond = exists(*order[k])
            if k == 4:
                pl.when(origin)(lambda: copies[8].start())
                cond = jnp.logical_and(cond, jnp.logical_not(origin))
            guarded(cond, lambda k=k: copies[k].start())

    def own():
        amplitude(8, 0, 0, L_OWN)
        out_ref[...] = migrate(8, L_OWN).reshape(PX, PY, NT)

    def meet():
        pl.semaphore_wait(barrier, count)
        pl.when(beside_route)(
            lambda: pl.semaphore_signal(near_sem, inc=1, device_id=device(0, 2), device_id_type=MESH)
        )

    make(0)

    @pl.when(quick)
    def _():
        meet()
        start(0)

    for c in range(L_Y + NOC - 1, NC):
        interpolate(c)
    pick(L_Y, LV)
    make(1)
    make(2)

    def start_far():
        pl.when(gx == 1)(lambda: start(0))
        pl.when(gx < 2)(lambda: start(2))
        pl.when(gx >= 2)(lambda: start(1))
        pl.when(gx != 1)(lambda: start(0))
        pl.when(gx < 2)(lambda: start(1))
        pl.when(gx >= 2)(lambda: start(2))

    @pl.when(middle)
    def _():
        meet()
        start_far()

    pl.when(quick)(lambda: start(1, 2))
    make(3)
    make(4)
    make(5)
    pl.when(route)(lambda: pl.semaphore_wait(near_sem, 1))
    pl.when(jnp.logical_not(early))(lambda: start(3, 4, 5))
    make(6)
    make(7)

    @pl.when(inner)
    def _():
        meet()
        start_far()

    @pl.when(early)
    def _():
        own()
        meet()
        start(0, 1, 2, 3, 4, 5)

    off_far = jnp.logical_and(has_far, jnp.logical_not(at_end))

    for dx, corner, near, k in ((-1, 1, 3, 6), (1, 2, 4, 7)):

        @pl.when(has_x[dx])
        def _(corner=corner, near=near, k=k):
            @pl.when(jnp.logical_not(beside))
            def _():
                copies[near].wait_recv()
                held[k - 6] += got[near].astype(F32)

            @pl.when(off_far)
            def _():
                copies[corner].wait_recv()
                held[k - 6] += got[corner].astype(F32)

            sent[k] = held[k - 6].astype(BF)
            copies[k].start()

    pl.when(jnp.logical_not(early))(own)

    @pl.when(late)
    def _():
        meet()
        start_far()

    def add(k):
        copies[k].wait_recv()
        out_ref[...] += got[k].astype(F32).reshape(PX, PY, NT)

    add(5)
    pl.when(off_far)(lambda: add(0))
    pl.when(has_x[1])(lambda: add(6))
    pl.when(has_x[-1])(lambda: add(7))
    pl.when(across)(lambda: add(8))

    @pl.when(route)
    def _():
        add(0)
        pl.when(has_x[1])(lambda: add(1))
        pl.when(has_x[-1])(lambda: add(2))

    for k, n in enumerate(order):
        cond = exists(*n)
        if k == 4:
            pl.when(origin)(lambda: copies[8].wait_send())
            cond = jnp.logical_and(cond, jnp.logical_not(origin))
        guarded(cond, lambda k=k: copies[k].wait_send())


def per_device(traces, aperture, geometry, trace_weight, class_weight, traveltime):
    hbm = pl.BlockSpec(memory_space=pltpu.HBM)
    tile = (PTS, NT)
    return pl.pallas_call(
        kernel,
        out_shape=jax.ShapeDtypeStruct((PX, PY, NT), F32),
        in_specs=[hbm] * 6,
        out_specs=pl.BlockSpec(memory_space=pltpu.VMEM),
        scratch_shapes=[
            pltpu.VMEM((NJ, NS), BF),
            pltpu.SMEM((2, 2, 9), jnp.int32),
            pltpu.VMEM((2, 3, 2, TR), jnp.int32),
            pltpu.VMEM((2, 2, TR), BF),
            pltpu.SMEM((NC,), F32),
            pltpu.VMEM((NC, NT), jnp.int32),
            pltpu.VMEM((NC, NS, NT), BF),
            pltpu.VMEM((NC, NJ, NT), BF),
            pltpu.VMEM((LV * NJ, NT), BF),
            pltpu.VMEM((9, PTS, LV * NJ), BF),
            pltpu.VMEM((2,) + tile, F32),
            pltpu.VMEM((8,) + tile, BF),
            pltpu.VMEM((9,) + tile, BF),
            pltpu.SemaphoreType.DMA((6,)),
            pltpu.SemaphoreType.DMA((9,)),
            pltpu.SemaphoreType.DMA((9,)),
            pltpu.SemaphoreType.REGULAR,
        ],
        compiler_params=pltpu.CompilerParams(
            collective_id=0, has_side_effects=True, vmem_limit_bytes=32 * 1024 * 1024
        ),
        cost_estimate=pl.CostEstimate(flops=3_000_000_000, bytes_accessed=2_000_000, transcendentals=0),
        name="migrate",
    )(
        *(
            pltpu.with_memory_space_constraint(x, pltpu.HBM)
            for x in (
                traces.reshape(NJ, NS),
                aperture,
                geometry.transpose(0, 2, 1, 3),
                trace_weight,
                class_weight,
                traveltime,
            )
        )
    )


def solution(mesh):
    return jax.shard_map(
        per_device,
        mesh=mesh,
        in_specs=(
            P("gx", "gy", None, None),
            P("gx", "gy", None),
            P("gx", "gy", None, None),
            P("gx", "gy", None),
            P(),
            P(),
        ),
        out_specs=P("gx", "gy", None),
        check_vma=False,
    )
```
